32 devices in a mesh: row: 8 (over z, x), col: 4 (over y, core).
Axes of the slice: x: 2, y: 2, z: 4, core: 2. Of those that a mesh axis runs over, the one named last changes fastest.
Arguments:
- density_first: bfloat16 [12288, 12288], P('row', 'col'), may hold values from -0.0068359375 to 0.0068359375
- density_second: bfloat16 [12288, 12288], P('row', 'col'), may hold values from -0.0068359375 to 0.0068359375
- basis: bfloat16 [64, 4096, 896], P(('row', 'col')), may hold values from -6 to 6
- tile_list: int32 [64, 7], P(('row', 'col')), may hold values from 0 to 95, as said below
- tile_count: int32 [64], P(('row', 'col')), may hold values from 5 to 7, as said below
- point_count: int32 [64], P(('row', 'col')), may hold values from 1024 to 4096, as said below
- offsets: float32 [3, 64, 4096], P(None, ('row', 'col')), may hold values from -5 to 5
- weights: float32 [64, 4096], P(('row', 'col')), may hold values from 0.05 to 1
- atom_of_point: int32 [64, 4096], P(('row', 'col')), may hold values from 0 to 1023, as said below
Outputs:
- density: float32 [2, 64, 4096], P(None, ('row', 'col'))
- moments: float32 [2, 9, 1024], replicated
The draws below stay inside these ranges and needn't reach their ends.
Inputs may be any that keep to these rules, and one draw needn't show every extreme that they name: `tile_list`: the 7 tile numbers of each batch are 7 consecutive numbers in some order. `tile_count`: some batch has 7. `point_count`: some batch has 4096. `atom_of_point`: the points of batch g belong to atoms (g * 16 + j) mod 1024 with j from 0 to 7.
All inputs are finite; a program needn't handle non-finite values.
Results may differ from the reference program's by a relative error of at most 0.0003.
Values may be sent and summed in bfloat16 or wider, within the bound.
A program may use at most 192 MiB of HBM per device.

```python
import math
import jax
import jax.numpy as jnp
from jax import lax

TILE = 128
NB = 12288
KT = 7
PTS = 4096
ATOMS = 1024
NT = 96
BATCHES = 64
N_ROW = 8
N_COL = 4


def lift_one(key, values, top):
    chosen = jax.random.randint(jax.random.fold_in(key, 17), (), 0, values.shape[0])
    return jnp.where(jnp.arange(values.shape[0]) == chosen, top, values).astype(jnp.int32)


def draw_tile_list(key, part):
    start_key = jax.random.fold_in(key, 3)
    order_key = jax.random.fold_in(key, 5)
    starts = jax.random.randint(start_key, (BATCHES, 1), 0, NT - KT + 1)
    order_keys = jax.random.split(order_key, BATCHES)
    orders = jax.vmap(lambda single: jax.random.permutation(single, KT))(order_keys)
    return (starts + orders).astype(jnp.int32)


def draw_tile_count(key, part):
    base = jax.random.randint(jax.random.fold_in(key, 7), (BATCHES,), KT - 2, KT + 1)
    return lift_one(key, base, KT)


def draw_point_count(key, part):
    base = jax.random.randint(jax.random.fold_in(key, 11), (BATCHES,), PTS // 4, PTS + 1)
    return lift_one(key, base, PTS)


def draw_atom_of_point(key, part):
    base = (jnp.arange(BATCHES, dtype=jnp.int32) * ATOMS // BATCHES)[:, None]
    spread = jax.random.randint(jax.random.fold_in(key, 13), (BATCHES, PTS), 0, 8)
    return ((base + spread) % ATOMS).astype(jnp.int32)


def level_of(own_key, extent, pieces, low, largest):
    def one(dim, blocks):
        steps = jax.random.uniform(jax.random.fold_in(jax.random.fold_in(own_key, 6), dim), (blocks,), jnp.float32, low / len(pieces), largest / len(pieces))
        return jnp.repeat(jnp.exp(steps), extent[dim] // blocks).reshape((-1,) + (1,) * (len(extent) - dim - 1))

    gain = one(*pieces[0])
    for cut in pieces[1:]:
        gain = gain * one(*cut)
    return gain


def normal_values(key, dims, scale, reach, pieces=(), kind=jnp.bfloat16):
    entries = jax.random.normal(key, dims, jnp.float32) * scale
    if len(pieces) > 0:
        entries = level_of(key, dims, pieces, -0.22, 0.18) * entries
    return jnp.clip(entries, min=-reach, max=reach).astype(kind)


def setup_inputs(seed: int = 0) -> dict:
    seeds = jax.random.split(jax.random.key(seed), 10)
    density_first = normal_values(seeds[0], (NB, NB), ((KT * TILE) ** 2) ** -0.5, 0.0068359375, ((0, 8), (1, 4)))
    density_second = normal_values(seeds[1], (NB, NB), ((KT * TILE) ** 2) ** -0.5, 0.0068359375, ((0, 8), (1, 4)))
    basis = normal_values(seeds[2], (BATCHES, PTS, KT * TILE), 1.0, 6.0, ((0, 32),))
    tile_list = draw_tile_list(jax.random.fold_in(seeds[9], 71), 0)
    tile_count = draw_tile_count(jax.random.fold_in(seeds[9], 71), 0)
    point_count = draw_point_count(jax.random.fold_in(seeds[9], 71), 0)
    offsets = normal_values(seeds[6], (3, BATCHES, PTS), 1.0, 5.0, ((1, 32),), jnp.float32)
    weights = jnp.clip(jnp.exp(math.log(1.0) - 2.9957323 * jax.random.uniform(seeds[7], (BATCHES, PTS), jnp.float32) ** level_of(seeds[7], (BATCHES, PTS), ((0, 32),), -0.2, 0.2)), 0.05, 1.0)
    atom_of_point = draw_atom_of_point(jax.random.fold_in(seeds[9], 71), 0)
    return dict(density_first=density_first, density_second=density_second, basis=basis, tile_list=tile_list, tile_count=tile_count, point_count=point_count, offsets=offsets, weights=weights, atom_of_point=atom_of_point)


def harmonics(offsets):
    first_axis = offsets[0]
    second_axis = offsets[1]
    third_axis = offsets[2]
    radius_sq = first_axis * first_axis + second_axis * second_axis + third_axis * third_axis
    return jnp.stack([jnp.ones_like(first_axis), first_axis, second_axis, third_axis,
                      first_axis * second_axis, second_axis * third_axis,
                      3.0 * third_axis * third_axis - radius_sq,
                      first_axis * third_axis,
                      first_axis * first_axis - second_axis * second_axis])


def storage_index(tiles, parts):
    per_part = NT // parts
    return ((tiles % parts) * per_part + tiles // parts).astype(jnp.int32)


def batch_density(stored_first, stored_second, values, tiles, live_tiles, live_points):
    inside = jnp.arange(TILE, dtype=jnp.int32)[None, :]
    rows = (storage_index(tiles, N_ROW)[:, None] * TILE + inside).reshape(-1)
    cols = (storage_index(tiles, N_COL)[:, None] * TILE + inside).reshape(-1)
    col_mask = jnp.repeat((jnp.arange(KT) < live_tiles).astype(jnp.bfloat16), TILE)
    masked = values * col_mask[None, :]
    point_mask = (jnp.arange(PTS) < live_points).astype(jnp.float32)
    results = []
    for stored in (stored_first, stored_second):
        block = stored[rows[:, None], cols[None, :]]
        product = jnp.dot(masked, block, preferred_element_type=jnp.float32)
        results.append(jnp.sum(product * masked.astype(jnp.float32), axis=1) * point_mask)
    return jnp.stack(results)


def reference(density_first, density_second, basis, tile_list, tile_count, point_count, offsets, weights, atom_of_point):
    def per_batch(inputs):
        values, tiles, live_tiles, live_points = inputs
        return batch_density(density_first, density_second, values, tiles, live_tiles, live_points)

    stacked = lax.map(per_batch, (basis, tile_list, tile_count, point_count))
    density = jnp.transpose(stacked, (1, 0, 2))
    harmonic = harmonics(offsets)
    moment_terms = density[:, None] * (weights[None, None] * harmonic[None])
    flat_terms = moment_terms.reshape(2 * 9, -1).T
    summed = jax.ops.segment_sum(flat_terms, atom_of_point.reshape(-1), num_segments=ATOMS)
    moments = summed.T.reshape(2, 9, ATOMS)
    return density, moments
```

```python
import functools

import jax
import jax.numpy as jnp
from jax import lax
from jax.experimental import pallas as pl
from jax.experimental.pallas import tpu as pltpu
from jax.sharding import PartitionSpec as P

TILE = 128
ATOMS = 1024
SPREAD = 8
TERMS = 9
SLOT = 16
SIGNS = (1, -1)
LEVELS = 32767.0
MESH = pl.DeviceIdType.MESH


def greet_all(me, peers, device):
    barrier = pltpu.get_barrier_semaphore()

    def greet(hop, carry):
        pl.semaphore_signal(
            barrier, inc=1, device_id=device((me + hop) % peers), device_id_type=MESH
        )
        return carry

    lax.fori_loop(1, peers, greet, 0)
    pl.semaphore_wait(barrier, peers - 1)


def fold_kernel(
    run, row_count, col_count, lists, first, second, folded, scales, starts,
    near, across, beside, behind, held, near_sem, recv_sem, send_sem, list_send, list_recv, self_sem,
):
    half = run // 2
    peers = row_count * col_count
    my_row = lax.axis_index("row")
    my_col = lax.axis_index("col")
    me = my_row * col_count + my_col
    matrices = (first, second)
    slots = near.shape[1]
    tiles = slots * row_count
    shares = [(sign * (my_col - my_row) + row_count * col_count) % col_count for sign in SIGNS]

    def device(index):
        return (index // col_count, index % col_count)

    def tile_of(d, tile_row, tile_col):
        rows = pl.ds(pl.multiple_of((tile_row // row_count) * TILE, TILE), TILE)
        cols = pl.ds(pl.multiple_of((tile_col // col_count) * TILE, TILE), TILE)
        return matrices[d].at[rows, cols]

    for d, sign in enumerate(SIGNS):

        def take(i, carry):
            mine = my_row + row_count * i
            other = (mine + sign * shares[d] + tiles) % tiles
            pltpu.make_async_copy(tile_of(d, mine, other), near.at[d, i], near_sem.at[d]).start()
            return carry

        lax.fori_loop(0, slots, take, 0)

    greet_all(me, peers, device)

    def list_copy(hop, place):
        return pltpu.make_async_remote_copy(
            src_ref=lists, dst_ref=held.at[place], send_sem=list_send.at[hop],
            recv_sem=list_recv.at[hop], device_id=device((me + hop) % peers), device_id_type=MESH,
        )

    def list_start(hop, carry):
        list_copy(hop, me).start()
        return carry

    def list_finish(hop, carry):
        list_copy(hop, (me + peers - hop) % peers).wait_recv()
        list_copy(hop, me).wait_send()
        return carry

    own_list = pltpu.make_async_copy(lists, held.at[me], self_sem)
    own_list.start()

    messages = []
    for e in range(1, half + 1):
        for d, sign in enumerate(SIGNS):
            to_row = (my_row - sign * e + 2 * row_count) % row_count
            messages.append((d, 0, e, to_row % col_count == my_col, to_row, (to_row + sign * e + col_count) % col_count))
            to_row = (my_row - sign * (e - run) + 2 * row_count) % row_count
            messages.append((d, 2, e, to_row % col_count == my_col, to_row, (to_row + sign * e + col_count) % col_count))
    for e in range(1, half + 1):
        for d, sign in enumerate(SIGNS):
            to_col = (my_col + sign * run + 2 * run * col_count) % col_count
            held_by = (sign * (to_col - my_row) + row_count * col_count) % col_count
            messages.append((d, 1, e, held_by == e, my_row, to_col))
    landings = (across, beside, behind)

    for d, kind, e, sends, to_row, to_col in messages:
        sign = SIGNS[d]
        place = (d * 3 + kind) * half + e - 1

        @pl.when(sends)
        def _():
            def send(i, carry):
                theirs = to_row + row_count * i
                shift = sign * e if kind == 0 else sign * (e - run)
                other = (theirs + shift + tiles) % tiles
                source = tile_of(d, theirs, other) if kind == 1 else tile_of(d, other, theirs)
                pltpu.make_async_remote_copy(
                    src_ref=source, dst_ref=landings[kind].at[d, i],
                    send_sem=send_sem.at[place], recv_sem=recv_sem.at[d * 3 + kind],
                    device_id=(to_row, to_col), device_id_type=MESH,
                ).start()
                return carry

            lax.fori_loop(0, slots, send, 0)

    lax.fori_loop(1, peers, list_start, 0)

    def keep(value, slot, d):
        top = jnp.maximum(jnp.max(jnp.abs(value), axis=0, keepdims=True), 1e-30)
        coded = jnp.round(value * (LEVELS / top))
        folded[slot, d] = coded.astype(jnp.int32).astype(jnp.int16)
        scales[slot, d:d + 1, :] = top * (1.0 / LEVELS)

    for d in range(2):
        pltpu.make_async_copy(near.at[d], near.at[d], near_sem.at[d]).wait()

        @pl.when(shares[d] == 0)
        def _():
            def plain(i, carry):
                keep(near[d, i].astype(jnp.float32), 2 * i, d)
                return carry

            lax.fori_loop(0, slots, plain, 0)

        @pl.when(jnp.logical_and(shares[d] >= 1, shares[d] <= half))
        def _():
            for kind in range(3):
                pltpu.make_async_copy(
                    landings[kind].at[d], landings[kind].at[d], recv_sem.at[d * 3 + kind]
                ).wait()

            def pair(i, carry):
                keep(near[d, i].astype(jnp.float32) + across[d, i].astype(jnp.float32).T, 2 * i, d)
                keep(beside[d, i].astype(jnp.float32) + behind[d, i].astype(jnp.float32).T, 2 * i + 1, d)
                return carry

            lax.fori_loop(0, slots, pair, 0)

    own_list.wait()
    lax.fori_loop(1, peers, list_finish, 0)
    lists_in = held[...]
    lane = lax.broadcasted_iota(jnp.int32, lists_in.shape, 2)
    smallest = jnp.min(jnp.where(lane < run, lists_in, tiles), axis=2, keepdims=True)
    starts[...] = jnp.broadcast_to(smallest, lists_in.shape)

    for d, kind, e, sends, to_row, to_col in messages:
        place = (d * 3 + kind) * half + e - 1

        @pl.when(sends)
        def _():
            pltpu.make_async_copy(near.at[d], near.at[d], send_sem.at[place]).wait()


def fold(lists, first, second, run, row_count, col_count):
    peers = row_count * col_count
    slots = first.shape[0] // TILE
    half = run // 2
    batches = lists.shape[0]
    band = pltpu.VMEM((2, slots, TILE, TILE), first.dtype)
    whole = pl.BlockSpec(memory_space=pltpu.VMEM)
    return pl.pallas_call(
        functools.partial(fold_kernel, run, row_count, col_count),
        out_shape=[
            jax.ShapeDtypeStruct((2 * slots, 2, TILE, TILE), jnp.int16),
            jax.ShapeDtypeStruct((2 * slots, 2, TILE), jnp.float32),
            jax.ShapeDtypeStruct((peers, batches, TILE), jnp.int32),
        ],
        in_specs=[whole, pl.BlockSpec(memory_space=pl.ANY), pl.BlockSpec(memory_space=pl.ANY)],
        out_specs=[whole] * 3,
        scratch_shapes=[
            band, band, band, band,
            pltpu.VMEM((peers, batches, TILE), jnp.int32),
            pltpu.SemaphoreType.DMA((2,)),
            pltpu.SemaphoreType.DMA((6,)),
            pltpu.SemaphoreType.DMA((6 * half,)),
            pltpu.SemaphoreType.DMA((peers,)),
            pltpu.SemaphoreType.DMA((peers,)),
            pltpu.SemaphoreType.DMA,
        ],
        compiler_params=pltpu.CompilerParams(
            collective_id=0, has_side_effects=True, vmem_limit_bytes=60 * 1024 * 1024
        ),
        name="fold",
    )(lists, first, second)


def pack_kernel(
    run, row_count, col_count, starts, place, tile_list, tile_count, folded, scales,
    out, out_scales, spots, sources, alive,
):
    slots = folded.shape[0] // 2
    half = run // 2
    batches, _, peers = out.shape[:3]
    my_row = place[0]
    my_col = place[1]

    def one(peer, carry):
        for b in range(batches):
            start = starts[peer, b, 0]
            mine = start + (my_row - start % row_count + row_count) % row_count
            slot = jnp.minimum(mine // row_count, slots - 1)
            for d, sign in enumerate(SIGNS):
                share = (sign * (my_col - my_row) + row_count * col_count) % col_count
                other = mine + sign * share
                far = jnp.logical_or(other < start, other >= start + run)
                index = 2 * slot + far.astype(jnp.int32)
                out[b, d, peer] = folded[index, d]
                out_scales[b, d, peer] = scales[index, d:d + 1, :]
        return carry

    lax.fori_loop(0, peers, one, 0)

    for b in range(batches):
        start = starts[my_row * col_count + my_col, b, 0]

        def find(j, carry):
            spots[b, tile_list[b, j] - start] = j
            return carry

        lax.fori_loop(0, run, find, 0)

        def table(k, carry):
            tile_row = (start + k) % row_count
            for d, sign in enumerate(SIGNS):
                for e in range(half + 1):
                    l = (k + sign * e + run) % run
                    tile_col = (tile_row + sign * e + col_count) % col_count
                    sources[b, d, k * (half + 1) + e] = tile_row * col_count + tile_col
                    last = jnp.maximum(spots[b, k], spots[b, l])
                    alive[b, d, k * (half + 1) + e] = jnp.where(last < tile_count[b], 1.0, 0.0)
            return carry

        lax.fori_loop(0, run, table, 0)


def pack(starts, tile_list, tile_count, folded, scales, row_count, col_count):
    run = tile_list.shape[1]
    peers, batches = starts.shape[:2]
    place = jnp.stack([lax.axis_index("row"), lax.axis_index("col")]).astype(jnp.int32)
    whole = pl.BlockSpec(memory_space=pltpu.VMEM)
    scalar = pl.BlockSpec(memory_space=pltpu.SMEM)
    return pl.pallas_call(
        functools.partial(pack_kernel, run, row_count, col_count),
        out_shape=[
            jax.ShapeDtypeStruct((batches, 2, peers, TILE, TILE), folded.dtype),
            jax.ShapeDtypeStruct((batches, 2, peers, 1, TILE), scales.dtype),
            jax.ShapeDtypeStruct((batches, run), jnp.int32),
            jax.ShapeDtypeStruct((batches, 2, run * (run // 2 + 1)), jnp.int32),
            jax.ShapeDtypeStruct((batches, 2, run * (run // 2 + 1)), jnp.float32),
        ],
        in_specs=[scalar] * 4 + [whole, whole],
        out_specs=[whole, whole, scalar, scalar, scalar],
        compiler_params=pltpu.CompilerParams(vmem_limit_bytes=60 * 1024 * 1024),
        name="pack",
    )(starts, place, tile_list, tile_count, folded, scales)


def density_kernel(
    run, row_count, col_count, spots, sources, alive, point_count, packed, packed_scales,
    basis, offsets, weights, atoms, density, every, *scratch,
):
    batches, points = weights.shape
    values, scratch = scratch[:batches], scratch[batches:]
    landed, scratch = scratch[:2 * batches], scratch[2 * batches:]
    (
        arrived_scales, blocks, sums, stage, held, basis_sem, send_sem, recv_sem, own_sem,
        scale_send, scale_recv, scale_own, last_send, last_recv, last_own,
    ) = scratch
    half = run // 2
    peers = row_count * col_count
    my_row = lax.axis_index("row")
    my_col = lax.axis_index("col")
    me = my_row * col_count + my_col
    chunk = min(512, points)
    stride = ATOMS // (peers * batches)
    pieces = [(b, d) for b in range(batches) for d in range(2)]

    def device(index):
        return (index // col_count, index % col_count)

    def load(b):
        for j in range(run):
            columns = pl.ds(j * TILE, TILE)
            pltpu.make_async_copy(basis.at[b, :, columns], values[b].at[j], basis_sem.at[b]).start()

    own = [pltpu.make_async_copy(packed.at[b, d, me], landed[b * 2 + d].at[me], own_sem.at[b * 2 + d]) for b, d in pieces]
    own_scales = pltpu.make_async_copy(packed_scales.at[:, :, me], arrived_scales.at[:, :, me], scale_own)
    own_scales.start()
    for copy in own:
        copy.start()
    greet_all(me, peers, device)

    def scale_start(hop, carry):
        to = (me + hop) % peers
        pltpu.make_async_remote_copy(
            src_ref=packed_scales.at[:, :, to], dst_ref=arrived_scales.at[:, :, me],
            send_sem=scale_send, recv_sem=scale_recv,
            device_id=device(to), device_id_type=MESH,
        ).start()
        return carry

    def start_piece(b, d):
        def send(hop, carry):
            to = (me + hop) % peers
            pltpu.make_async_remote_copy(
                src_ref=packed.at[b, d, to], dst_ref=landed[b * 2 + d].at[me],
                send_sem=send_sem.at[b * 2 + d], recv_sem=recv_sem.at[b * 2 + d],
                device_id=device(to), device_id_type=MESH,
            ).start()
            return carry

        lax.fori_loop(1, peers, send, 0)

    def wait_bytes(ref, sem):
        pltpu.make_async_copy(ref, ref, sem).wait()

    start_piece(*pieces[0])
    lax.fori_loop(1, peers, scale_start, 0)
    start_piece(*pieces[1])
    for b in range(batches):
        load(b)
    own_scales.wait()
    wait_bytes(arrived_scales.at[:, :, pl.ds(0, peers - 1)], scale_recv)
    sums[...] = jnp.zeros_like(sums)

    for index, (b, d) in enumerate(pieces):
        sign = SIGNS[d]
        own[index].wait()
        wait_bytes(landed[index].at[pl.ds(0, peers - 1)], recv_sem.at[index])
        if index + 2 < len(pieces):
            start_piece(*pieces[index + 2])
        if d == 0:
            wait_bytes(values[b], basis_sem.at[b])

        for k in range(run):
            for e in range(half + 1):
                peer = sources[b, d, k * (half + 1) + e]
                scale = arrived_scales[b, d, peer] * alive[b, d, k * (half + 1) + e]
                tile = landed[index][peer].astype(jnp.int32).astype(jnp.float32) * scale
                high = tile.astype(jnp.bfloat16)
                low = (tile - high.astype(jnp.float32)).astype(jnp.bfloat16)
                blocks[k, 0:TILE, e * TILE:(e + 1) * TILE] = high
                blocks[k, TILE:2 * TILE, e * TILE:(e + 1) * TILE] = low

        def some(c, carry):
            begin = pl.multiple_of(c * chunk, chunk)
            rows = pl.ds(begin, chunk)
            parts = [values[b][spots[b, k], rows, :] for k in range(run)]
            total = None
            for k in range(run):
                product = jnp.dot(
                    jnp.concatenate([parts[k], parts[k]], axis=1), blocks[k],
                    preferred_element_type=jnp.float32,
                )
                for e in range(half + 1):
                    part = product[:, e * TILE:(e + 1) * TILE] * parts[(k + sign * e) % run].astype(jnp.float32)
                    total = part if total is None else total + part
            row = jnp.sum(total.T, axis=0, keepdims=True)
            spot = begin + lax.broadcasted_iota(jnp.int32, (1, chunk), 1)
            row = jnp.where(spot < point_count[b], row, 0.0)
            density[d, b:b + 1, rows] = row
            x = offsets[0, b:b + 1, rows]
            y = offsets[1, b:b + 1, rows]
            z = offsets[2, b:b + 1, rows]
            w = weights[b:b + 1, rows]
            r2 = x * x + y * y + z * z
            weighted = [
                w, w * x, w * y, w * z, w * (x * y), w * (y * z),
                w * (3.0 * z * z - r2), w * (x * z), w * (x * x - y * y),
            ]
            terms = [row * item for item in weighted]
            terms += [jnp.zeros((1, chunk), jnp.float32)] * (SLOT - len(terms))
            stacked = jnp.concatenate(terms, axis=0)
            base = (me * batches + b) * stride
            atom = (atoms[b:b + 1, rows] - base + ATOMS) % ATOMS
            for j in range(SPREAD):
                chosen = jnp.where(atom == j, stacked, 0.0)
                partial = None
                for q in range(chunk // TILE):
                    part = chosen[:, q * TILE:(q + 1) * TILE]
                    partial = part if partial is None else partial + part
                at_rows = pl.ds(j * SLOT, SLOT)
                sums[index, at_rows, :] = sums[index, at_rows, :] + partial
            return carry

        lax.fori_loop(0, points // chunk, some, 0)

    for index in range(len(pieces)):
        stage[index:index + 1, :] = jnp.sum(sums[index].T, axis=0, keepdims=True)
    for index, (b, d) in enumerate(pieces):
        wait_bytes(landed[index].at[pl.ds(0, peers - 1)], send_sem.at[index])
    wait_bytes(arrived_scales.at[:, :, pl.ds(0, peers - 1)], scale_send)

    def last_start(hop, carry):
        pltpu.make_async_remote_copy(
            src_ref=stage, dst_ref=held.at[me], send_sem=last_send, recv_sem=last_recv,
            device_id=device((me + hop) % peers), device_id_type=MESH,
        ).start()
        return carry

    lax.fori_loop(1, peers, last_start, 0)
    last = pltpu.make_async_copy(stage, held.at[me], last_own)
    last.start()
    last.wait()
    wait_bytes(held.at[pl.ds(0, peers - 1)], last_recv)
    every[...] = held[...]
    wait_bytes(held.at[pl.ds(0, peers - 1)], last_send)


def density_of(
    spots, sources, alive, point_count, packed, packed_scales, basis, offsets, weights, atoms,
    row_count, col_count,
):
    batches, points, span = basis.shape
    run = span // TILE
    half = run // 2
    peers = row_count * col_count
    whole = pl.BlockSpec(memory_space=pltpu.VMEM)
    scalar = pl.BlockSpec(memory_space=pltpu.SMEM)
    anywhere = pl.BlockSpec(memory_space=pl.ANY)
    pieces = 2 * batches
    return pl.pallas_call(
        functools.partial(density_kernel, run, row_count, col_count),
        out_shape=[
            jax.ShapeDtypeStruct((2, batches, points), jnp.float32),
            jax.ShapeDtypeStruct((peers, pieces, SPREAD * SLOT), jnp.float32),
        ],
        in_specs=[scalar] * 4 + [anywhere, anywhere, anywhere, whole, whole, whole],
        out_specs=[whole, whole],
        scratch_shapes=[pltpu.VMEM((run, points, TILE), basis.dtype)] * batches
        + [pltpu.VMEM(packed.shape[2:], packed.dtype)] * pieces
        + [
            pltpu.VMEM(packed_scales.shape, packed_scales.dtype),
            pltpu.VMEM((run, 2 * TILE, (half + 1) * TILE), jnp.bfloat16),
            pltpu.VMEM((pieces, SPREAD * SLOT, TILE), jnp.float32),
            pltpu.VMEM((pieces, SPREAD * SLOT), jnp.float32),
            pltpu.VMEM((peers, pieces, SPREAD * SLOT), jnp.float32),
            pltpu.SemaphoreType.DMA((batches,)),
            pltpu.SemaphoreType.DMA((pieces,)),
            pltpu.SemaphoreType.DMA((pieces,)),
            pltpu.SemaphoreType.DMA((pieces,)),
            pltpu.SemaphoreType.DMA,
            pltpu.SemaphoreType.DMA,
            pltpu.SemaphoreType.DMA,
            pltpu.SemaphoreType.DMA,
            pltpu.SemaphoreType.DMA,
            pltpu.SemaphoreType.DMA,
        ],
        compiler_params=pltpu.CompilerParams(
            collective_id=1, has_side_effects=True, vmem_limit_bytes=62 * 1024 * 1024
        ),
        name="density",
    )(spots, sources, alive, point_count, packed, packed_scales, basis, offsets, weights, atoms)


def local(
    density_first, density_second, basis, tile_list, tile_count, point_count, offsets, weights,
    atom_of_point,
):
    row_count = lax.axis_size("row")
    col_count = lax.axis_size("col")
    peers = row_count * col_count
    batches, run = tile_list.shape
    lists = jnp.pad(tile_list, ((0, 0), (0, TILE - run)))
    folded, scales, starts = fold(lists, density_first, density_second, run, row_count, col_count)
    packed, packed_scales, spots, sources, alive = pack(
        starts, tile_list, tile_count, folded, scales, row_count, col_count
    )
    density, every = density_of(
        spots, sources, alive, point_count, packed, packed_scales, basis, offsets, weights,
        atom_of_point, row_count, col_count,
    )
    stride = ATOMS // (peers * batches)
    every = every.reshape(peers, batches, 2, SPREAD, SLOT)[..., :TERMS]
    every = every.transpose(2, 4, 0, 1, 3).reshape(2 * TERMS, peers * batches, SPREAD)
    blocks = -(-SPREAD // stride)
    every = jnp.pad(every, ((0, 0), (0, 0), (0, blocks * stride - SPREAD)))
    total = None
    for q in range(blocks):
        part = every[:, :, q * stride:(q + 1) * stride].reshape(2 * TERMS, ATOMS)
        part = jnp.roll(part, q * stride, axis=1)
        total = part if total is None else total + part
    return density, total.reshape(2, TERMS, ATOMS)


def solution(mesh):
    placed = (
        P("row", "col"),
        P("row", "col"),
        P(("row", "col"), None, None),
        P(("row", "col"), None),
        P(("row", "col")),
        P(("row", "col")),
        P(None, ("row", "col"), None),
        P(("row", "col"), None),
        P(("row", "col"), None),
    )
    return jax.shard_map(
        local,
        mesh=mesh,
        in_specs=placed,
        out_specs=(P(None, ("row", "col"), None), P()),
        check_vma=False,
    )
```

```python
import functools

import jax
import jax.numpy as jnp
from jax import lax
from jax.experimental import pallas as pl
from jax.experimental.pallas import tpu as pltpu
from jax.sharding import PartitionSpec as P

TILE = 128
ATOMS = 1024
SPREAD = 8
TERMS = 9
SLOT = 16
SIGNS = (1, -1)
LEVELS = 32767.0
MESH = pl.DeviceIdType.MESH


def greet_all(me, peers, device):
    barrier = pltpu.get_barrier_semaphore()

    def greet(hop, carry):
        pl.semaphore_signal(
            barrier, inc=1, device_id=device((me + hop) % peers), device_id_type=MESH
        )
        return carry

    lax.fori_loop(1, peers, greet, 0)
    pl.semaphore_wait(barrier, peers - 1)


def prep_kernel(run, row_count, tile_list, tile_count, lists, spots, others, alive, order):
    batches = tile_list.shape[0]
    width = run // 2 + 1
    lane = lax.broadcasted_iota(jnp.int32, lists.shape, 1)
    starts = jnp.zeros(lists.shape, jnp.int32)
    for b in range(batches):
        start = functools.reduce(jnp.minimum, [tile_list[b, j] for j in range(run)])
        starts = jnp.where(lane == b, start, starts)

        def find(j, carry):
            order[tile_list[b, j] - start] = j
            return carry

        lax.fori_loop(0, run, find, 0)

        def table(r, carry):
            offset = (r + row_count - start % row_count) % row_count
            k = jnp.minimum(offset, run - 1)
            spots[b, r] = order[k]
            for d, sign in enumerate(SIGNS):
                for e in range(width):
                    other = order[(k + sign * e + run) % run]
                    live = jnp.logical_and(offset < run, jnp.maximum(order[k], other) < tile_count[b])
                    others[b, d, r * width + e] = other
                    alive[b, d, r * width + e] = jnp.where(live, 1.0, 0.0)
            return carry

        lax.fori_loop(0, row_count, table, 0)
    lists[...] = starts


def prep(tile_list, tile_count, row_count):
    batches, run = tile_list.shape
    width = run // 2 + 1
    scalar = pl.BlockSpec(memory_space=pltpu.SMEM)
    return pl.pallas_call(
        functools.partial(prep_kernel, run, row_count),
        out_shape=[
            jax.ShapeDtypeStruct((1, TILE), jnp.int32),
            jax.ShapeDtypeStruct((batches, row_count), jnp.int32),
            jax.ShapeDtypeStruct((batches, 2, row_count * width), jnp.int32),
            jax.ShapeDtypeStruct((batches, 2, row_count * width), jnp.float32),
        ],
        in_specs=[scalar, scalar],
        out_specs=[pl.BlockSpec(memory_space=pltpu.VMEM), scalar, scalar, scalar],
        scratch_shapes=[pltpu.SMEM((run,), jnp.int32)],
        name="prep",
    )(tile_list, tile_count)


def main_kernel(
    run, row_count, col_count, spots, others, alive, point_count, lists, first, second, basis,
    offsets, weights, atoms, density, every, *scratch,
):
    batches, points = weights.shape
    pieces = [(b, d) for d in range(2) for b in range(batches)]
    values, scratch = scratch[:batches], scratch[batches:]
    outbox, scratch = scratch[:len(pieces)], scratch[len(pieces):]
    landed, scratch = scratch[:len(pieces)], scratch[len(pieces):]
    folded, fold_scales, out_scales, land_scales, scratch = (
        scratch[0:2], scratch[2:4], scratch[4:6], scratch[6:8], scratch[8:]
    )
    (
        near, across, beside, behind, held, starts, blocks, running, sums, stage, gathered,
        near_sem, fold_recv, fold_send, list_send, list_recv, list_own, basis_sem,
        send_sem, recv_sem, own_sem, scale_send, scale_recv, scale_own,
        last_send, last_recv, last_own,
    ) = scratch
    half = run // 2
    width = half + 1
    peers = row_count * col_count
    my_row = lax.axis_index("row")
    my_col = lax.axis_index("col")
    me = my_row * col_count + my_col
    matrices = (first, second)
    slots = near.shape[1]
    tiles = slots * row_count
    side = row_count // 2
    my_side = my_row // side
    chunk = min(512, points)
    stride = ATOMS // (peers * batches)
    shares = [(sign * (my_col - my_row) + row_count * col_count) % col_count for sign in SIGNS]

    def device(index):
        return (index // col_count, index % col_count)

    def wait_bytes(ref, sem):
        pltpu.make_async_copy(ref, ref, sem).wait()

    def tile_of(d, tile_row, tile_col):
        rows = pl.ds(pl.multiple_of((tile_row // row_count) * TILE, TILE), TILE)
        cols = pl.ds(pl.multiple_of((tile_col // col_count) * TILE, TILE), TILE)
        return matrices[d].at[rows, cols]

    for d, sign in enumerate(SIGNS):

        def take(i, carry):
            mine = my_row + row_count * i
            other = (mine + sign * shares[d] + tiles) % tiles
            pltpu.make_async_copy(tile_of(d, mine, other), near.at[d, i], near_sem.at[d]).start()
            return carry

        lax.fori_loop(0, slots, take, 0)

    own_list = pltpu.make_async_copy(lists, held.at[me], list_own)
    own_list.start()
    greet_all(me, peers, device)

    def list_start(hop, carry):
        pltpu.make_async_remote_copy(
            src_ref=lists, dst_ref=held.at[me], send_sem=list_send, recv_sem=list_recv,
            device_id=device((me + hop) % peers), device_id_type=MESH,
        ).start()
        return carry

    lax.fori_loop(1, peers, list_start, 0)

    messages = []
    for d, sign in enumerate(SIGNS):
        for e in range(1, half + 1):
            for kind, shift in ((0, sign * e), (2, sign * (e - run))):
                to_row = (my_row - shift + 2 * row_count) % row_count
                to_col = (to_row + sign * e + col_count) % col_count
                messages.append((d, kind, e, to_row % col_count == my_col, to_row, to_col))
        for e in range(1, half + 1):
            to_col = (my_col + sign * run + 2 * run * col_count) % col_count
            share = (sign * (to_col - my_row) + row_count * col_count) % col_count
            messages.append((d, 1, e, share == e, my_row, to_col))
    landings = (across, beside, behind)

    for d, kind, e, sends, to_row, to_col in messages:
        sign = SIGNS[d]
        place = (d * 3 + kind) * half + e - 1

        @pl.when(sends)
        def _():
            def send(i, carry):
                theirs = to_row + row_count * i
                shift = sign * e if kind == 0 else sign * (e - run)
                other = (theirs + shift + tiles) % tiles
                source = tile_of(d, theirs, other) if kind == 1 else tile_of(d, other, theirs)
                pltpu.make_async_remote_copy(
                    src_ref=source, dst_ref=landings[kind].at[d, i],
                    send_sem=fold_send.at[place], recv_sem=fold_recv.at[d * 3 + kind],
                    device_id=(to_row, to_col), device_id_type=MESH,
                ).start()
                return carry

            lax.fori_loop(0, slots, send, 0)

    for b in range(batches):
        for j in range(run):
            columns = pl.ds(j * TILE, TILE)
            pltpu.make_async_copy(basis.at[b, :, columns], values[b].at[j], basis_sem.at[b]).start()

    own_list.wait()
    wait_bytes(held.at[pl.ds(0, peers - 1)], list_recv)
    to_scalars = pltpu.make_async_copy(held, starts, list_own)
    to_scalars.start()
    to_scalars.wait()

    def keep(value, d, slot):
        top = jnp.maximum(jnp.max(jnp.abs(value), axis=0, keepdims=True), 1e-30)
        folded[d][slot] = jnp.round(value * (LEVELS / top)).astype(jnp.int32).astype(jnp.int16)
        fold_scales[d][slot] = top * (1.0 / LEVELS)

    def fold(d):
        wait_bytes(near.at[d], near_sem.at[d])

        @pl.when(shares[d] == 0)
        def _():
            def plain(i, carry):
                value = near[d, i].astype(jnp.float32)
                keep(value, d, 2 * i)
                keep(value, d, 2 * i + 1)
                return carry

            lax.fori_loop(0, slots, plain, 0)

        @pl.when(jnp.logical_and(shares[d] >= 1, shares[d] <= half))
        def _():
            for kind in range(3):
                wait_bytes(landings[kind].at[d], fold_recv.at[d * 3 + kind])

            def pair(i, carry):
                keep(near[d, i].astype(jnp.float32) + across[d, i].astype(jnp.float32).T, d, 2 * i)
                keep(beside[d, i].astype(jnp.float32) + behind[d, i].astype(jnp.float32).T, d, 2 * i + 1)
                return carry

            lax.fori_loop(0, slots, pair, 0)

        if col_count > width:

            @pl.when(shares[d] > half)
            def _():
                folded[d][...] = jnp.zeros_like(folded[d])
                fold_scales[d][...] = jnp.zeros_like(fold_scales[d])

    def pack(d):
        sign = SIGNS[d]

        def one(peer, carry):
            for b in range(batches):
                start = starts[peer, 0, b]
                mine = start + (my_row + row_count - start % row_count) % row_count
                slot = jnp.minimum(mine // row_count, slots - 1)
                other = mine + sign * shares[d]
                inside = jnp.logical_and(other >= start, other < start + run)
                index = 2 * slot + jnp.where(inside, 0, 1)
                outbox[d * batches + b][peer] = folded[d][index]
                out_scales[d][peer, b:b + 1, :] = fold_scales[d][index]
            return carry

        lax.fori_loop(0, peers, one, 0)

    def send_scales(d):
        pltpu.make_async_copy(out_scales[d].at[me], land_scales[d].at[me], scale_own.at[d]).start()

        def send(hop, carry):
            to = (me + hop) % peers
            pltpu.make_async_remote_copy(
                src_ref=out_scales[d].at[to], dst_ref=land_scales[d].at[me],
                send_sem=scale_send.at[d], recv_sem=scale_recv.at[d],
                device_id=device(to), device_id_type=MESH,
            ).start()
            return carry

        lax.fori_loop(1, peers, send, 0)

    def send_piece(index):
        pltpu.make_async_copy(outbox[index].at[me], landed[index].at[me], own_sem.at[index]).start()

        def send(hop, carry):
            to = (me + hop) % peers
            far = ((to // col_count) // side + my_side) % 2
            pltpu.make_async_remote_copy(
                src_ref=outbox[index].at[to], dst_ref=landed[index].at[me],
                send_sem=send_sem.at[index], recv_sem=recv_sem.at[index * 2 + far],
                device_id=device(to), device_id_type=MESH,
            ).start()
            return carry

        lax.fori_loop(1, peers, send, 0)

    def compute(index, far):
        b, d = pieces[index]
        sign = SIGNS[d]
        low_row = ((my_side + far) % 2) * side

        for i in range(side):
            for e in range(width):
                row = low_row + i
                peer = row * col_count + (row + sign * e + col_count) % col_count
                scale = land_scales[d][peer, b:b + 1, :] * alive[b, d, row * width + e]
                tile = landed[index][peer].astype(jnp.int32).astype(jnp.float32) * scale
                high = tile.astype(jnp.bfloat16)
                low = (tile - high.astype(jnp.float32)).astype(jnp.bfloat16)
                blocks[i, 0:TILE, e * TILE:(e + 1) * TILE] = high
                blocks[i, TILE:2 * TILE, e * TILE:(e + 1) * TILE] = low

        def some(c, carry):
            begin = pl.multiple_of(c * chunk, chunk)
            rows = pl.ds(begin, chunk)
            total = running[rows, :] if far else None
            for i in range(side):
                row = low_row + i
                part = values[b][spots[b, row], rows, :]
                product = jnp.dot(
                    jnp.concatenate([part, part], axis=1), blocks[i],
                    preferred_element_type=jnp.float32,
                )
                for e in range(width):
                    other = values[b][others[b, d, row * width + e], rows, :] if e else part
                    term = product[:, e * TILE:(e + 1) * TILE] * other.astype(jnp.float32)
                    total = term if total is None else total + term
            if not far:
                running[rows, :] = total
                return carry
            line = jnp.sum(total.T, axis=0, keepdims=True)
            spot = begin + lax.broadcasted_iota(jnp.int32, (1, chunk), 1)
            line = jnp.where(spot < point_count[b], line, 0.0)
            density[d, b:b + 1, rows] = line
            x = offsets[0, b:b + 1, rows]
            y = offsets[1, b:b + 1, rows]
            z = offsets[2, b:b + 1, rows]
            w = weights[b:b + 1, rows]
            r2 = x * x + y * y + z * z
            weighted = [
                w, w * x, w * y, w * z, w * (x * y), w * (y * z),
                w * (3.0 * z * z - r2), w * (x * z), w * (x * x - y * y),
            ]
            terms = [line * item for item in weighted]
            terms += [jnp.zeros((1, chunk), jnp.float32)] * (SLOT - len(terms))
            stacked = jnp.concatenate(terms, axis=0)
            base = (me * batches + b) * stride
            atom = (atoms[b:b + 1, rows] - base + ATOMS) % ATOMS
            for j in range(SPREAD):
                chosen = jnp.where(atom == j, stacked, 0.0)
                partial = None
                for q in range(chunk // TILE):
                    part = chosen[:, q * TILE:(q + 1) * TILE]
                    partial = part if partial is None else partial + part
                at_rows = pl.ds(j * SLOT, SLOT)
                sums[index, at_rows, :] = sums[index, at_rows, :] + partial
            return carry

        lax.fori_loop(0, points // chunk, some, 0)

    sums[...] = jnp.zeros_like(sums)
    for d in range(2):
        fold(d)
        pack(d)
        send_scales(d)
        if d == 0:
            for b in range(batches):
                send_piece(b)

    for b in range(batches):
        wait_bytes(values[b], basis_sem.at[b])
    for index, (b, d) in enumerate(pieces):
        if b == 0:
            pltpu.make_async_copy(out_scales[d].at[me], land_scales[d].at[me], scale_own.at[d]).wait()
            wait_bytes(land_scales[d].at[pl.ds(0, peers - 1)], scale_recv.at[d])
        pltpu.make_async_copy(outbox[index].at[me], landed[index].at[me], own_sem.at[index]).wait()
        wait_bytes(landed[index].at[pl.ds(0, peers // 2 - 1)], recv_sem.at[index * 2])
        if index + batches < len(pieces):
            send_piece(index + batches)
        compute(index, 0)
        wait_bytes(landed[index].at[pl.ds(0, peers // 2)], recv_sem.at[index * 2 + 1])
        compute(index, 1)

    for index in range(len(pieces)):
        stage[index:index + 1, :] = jnp.sum(sums[index].T, axis=0, keepdims=True)
    for index in range(len(pieces)):
        wait_bytes(landed[index].at[pl.ds(0, peers - 1)], send_sem.at[index])
    for d in range(2):
        wait_bytes(land_scales[d].at[pl.ds(0, peers - 1)], scale_send.at[d])
    wait_bytes(held.at[pl.ds(0, peers - 1)], list_send)

    def last_start(hop, carry):
        pltpu.make_async_remote_copy(
            src_ref=stage, dst_ref=gathered.at[me], send_sem=last_send, recv_sem=last_recv,
            device_id=device((me + hop) % peers), device_id_type=MESH,
        ).start()
        return carry

    lax.fori_loop(1, peers, last_start, 0)
    last = pltpu.make_async_copy(stage, gathered.at[me], last_own)
    last.start()
    for d, kind, e, sends, to_row, to_col in messages:
        place = (d * 3 + kind) * half + e - 1

        @pl.when(sends)
        def _():
            wait_bytes(near.at[d], fold_send.at[place])

    last.wait()
    wait_bytes(gathered.at[pl.ds(0, peers - 1)], last_recv)
    every[...] = gathered[...]
    wait_bytes(gathered.at[pl.ds(0, peers - 1)], last_send)


def density_of(
    spots, others, alive, point_count, lists, first, second, basis, offsets, weights, atoms,
    row_count, col_count,
):
    batches, points, span = basis.shape
    run = span // TILE
    half = run // 2
    peers = row_count * col_count
    slots = first.shape[0] // TILE
    pieces = 2 * batches
    whole = pl.BlockSpec(memory_space=pltpu.VMEM)
    scalar = pl.BlockSpec(memory_space=pltpu.SMEM)
    anywhere = pl.BlockSpec(memory_space=pl.ANY)
    copies = pltpu.SemaphoreType.DMA
    return pl.pallas_call(
        functools.partial(main_kernel, run, row_count, col_count),
        out_shape=[
            jax.ShapeDtypeStruct((2, batches, points), jnp.float32),
            jax.ShapeDtypeStruct((peers, pieces, SPREAD * SLOT), jnp.float32),
        ],
        in_specs=[scalar] * 4 + [whole] + [anywhere] * 3 + [whole] * 3,
        out_specs=[whole, whole],
        scratch_shapes=[pltpu.VMEM((run, points, TILE), basis.dtype)] * batches
        + [pltpu.VMEM((peers, TILE, TILE), jnp.int16)] * (2 * pieces)
        + [pltpu.VMEM((2 * slots, TILE, TILE), jnp.int16)] * 2
        + [pltpu.VMEM((2 * slots, 1, TILE), jnp.float32)] * 2
        + [pltpu.VMEM((peers, batches, TILE), jnp.float32)] * 4
        + [pltpu.VMEM((2, slots, TILE, TILE), first.dtype)] * 4
        + [
            pltpu.VMEM((peers, 1, TILE), jnp.int32),
            pltpu.SMEM((peers, 1, TILE), jnp.int32),
            pltpu.VMEM((row_count // 2, 2 * TILE, (half + 1) * TILE), jnp.bfloat16),
            pltpu.VMEM((points, TILE), jnp.float32),
            pltpu.VMEM((pieces, SPREAD * SLOT, TILE), jnp.float32),
            pltpu.VMEM((pieces, SPREAD * SLOT), jnp.float32),
            pltpu.VMEM((peers, pieces, SPREAD * SLOT), jnp.float32),
            copies((2,)), copies((6,)), copies((6 * half,)), copies, copies, copies,
            copies((batches,)), copies((pieces,)), copies((2 * pieces,)), copies((pieces,)),
            copies((2,)), copies((2,)), copies((2,)), copies, copies, copies,
        ],
        compiler_params=pltpu.CompilerParams(
            collective_id=0, has_side_effects=True, vmem_limit_bytes=62 * 1024 * 1024
        ),
        name="density",
    )(spots, others, alive, point_count, lists, first, second, basis, offsets, weights, atoms)


def local(
    density_first, density_second, basis, tile_list, tile_count, point_count, offsets, weights,
    atom_of_point,
):
    row_count = lax.axis_size("row")
    col_count = lax.axis_size("col")
    peers = row_count * col_count
    batches = tile_list.shape[0]
    lists, spots, others, alive = prep(tile_list, tile_count, row_count)
    density, every = density_of(
        spots, others, alive, point_count, lists, density_first, density_second, basis, offsets,
        weights, atom_of_point, row_count, col_count,
    )
    stride = ATOMS // (peers * batches)
    every = every.reshape(peers, 2, batches, SPREAD, SLOT)[..., :TERMS]
    every = every.transpose(1, 4, 0, 2, 3).reshape(2 * TERMS, peers * batches, SPREAD)
    blocks = -(-SPREAD // stride)
    every = jnp.pad(every, ((0, 0), (0, 0), (0, blocks * stride - SPREAD)))
    total = None
    for q in range(blocks):
        part = every[:, :, q * stride:(q + 1) * stride].reshape(2 * TERMS, ATOMS)
        part = jnp.roll(part, q * stride, axis=1)
        total = part if total is None else total + part
    return density, total.reshape(2, TERMS, ATOMS)


def solution(mesh):
    placed = (
        P("row", "col"),
        P("row", "col"),
        P(("row", "col"), None, None),
        P(("row", "col"), None),
        P(("row", "col")),
        P(("row", "col")),
        P(None, ("row", "col"), None),
        P(("row", "col"), None),
        P(("row", "col"), None),
    )
    return jax.shard_map(
        local,
        mesh=mesh,
        in_specs=placed,
        out_specs=(P(None, ("row", "col"), None), P()),
        check_vma=False,
    )
```

```python
import functools

import jax
import jax.numpy as jnp
from jax import lax
from jax.experimental import pallas as pl
from jax.experimental.pallas import tpu as pltpu
from jax.sharding import PartitionSpec as P

TILE = 128
ATOMS = 1024
SPREAD = 8
TERMS = 9
SLOT = 16
SIGNS = (1, -1)
LEVELS = 32767.0
MESH = pl.DeviceIdType.MESH


def greet_all(me, peers, device):
    barrier = pltpu.get_barrier_semaphore()

    def greet(hop, carry):
        pl.semaphore_signal(
            barrier, inc=1, device_id=device((me + hop) % peers), device_id_type=MESH
        )
        return carry

    lax.fori_loop(1, peers, greet, 0)
    pl.semaphore_wait(barrier, peers - 1)


def main_kernel(
    run, row_count, col_count, tile_list, tile_count, point_count, first, second, basis,
    offsets, weights, atoms, density, every, *scratch,
):
    batches, points = weights.shape
    pieces = [(b, d) for d in range(2) for b in range(batches)]
    values, scratch = scratch[:batches], scratch[batches:]
    outbox, scratch = scratch[:len(pieces)], scratch[len(pieces):]
    landed, scratch = scratch[:len(pieces)], scratch[len(pieces):]
    folded, fold_scales, out_scales, land_scales, scratch = (
        scratch[0:2], scratch[2:4], scratch[4:6], scratch[6:8], scratch[8:]
    )
    (
        sources, alive, order, lists, fold_out, gather_sem,
        near, across, beside, behind, held, starts, blocks, sums, stage, gathered,
        near_sem, fold_recv, fold_send, list_send, list_recv, list_own, basis_sem,
        send_sem, recv_sem, own_sem, scale_send, scale_recv, scale_own,
        last_send, last_recv, last_own,
    ) = scratch
    half = run // 2
    width = half + 1
    peers = row_count * col_count
    my_row = lax.axis_index("row")
    my_col = lax.axis_index("col")
    me = my_row * col_count + my_col
    matrices = (first, second)
    slots = near.shape[1]
    tiles = slots * row_count
    chunk = min(512, points)
    stride = ATOMS // (peers * batches)
    shares = [(sign * (my_col - my_row) + row_count * col_count) % col_count for sign in SIGNS]

    def device(index):
        return (index // col_count, index % col_count)

    def wait_bytes(ref, sem):
        pltpu.make_async_copy(ref, ref, sem).wait()

    def tile_of(d, tile_row, tile_col):
        rows = pl.ds(pl.multiple_of((tile_row // row_count) * TILE, TILE), TILE)
        cols = pl.ds(pl.multiple_of((tile_col // col_count) * TILE, TILE), TILE)
        return matrices[d].at[rows, cols]

    for d, sign in enumerate(SIGNS):

        def take(i, carry):
            mine = my_row + row_count * i
            other = (mine + sign * shares[d] + tiles) % tiles
            pltpu.make_async_copy(tile_of(d, mine, other), near.at[d, i], near_sem.at[d]).start()
            return carry

        lax.fori_loop(0, slots, take, 0)

    lane = lax.broadcasted_iota(jnp.int32, lists.shape, 1)
    firsts = jnp.zeros(lists.shape, jnp.int32)
    begins = []
    for b in range(batches):
        begins.append(functools.reduce(jnp.minimum, [tile_list[b, j] for j in range(run)]))
        firsts = jnp.where(lane == b, begins[b], firsts)
    lists[...] = firsts

    messages = []
    for d, sign in enumerate(SIGNS):
        for e in range(1, half + 1):
            for kind, shift in ((0, sign * e), (2, sign * (e - run))):
                to_row = (my_row - shift + 2 * row_count) % row_count
                to_col = (to_row + sign * e + col_count) % col_count
                messages.append((d, kind, e, to_row % col_count == my_col, to_row, to_col))
        for e in range(1, half + 1):
            to_col = (my_col + sign * run + 2 * run * col_count) % col_count
            share = (sign * (to_col - my_row) + row_count * col_count) % col_count
            messages.append((d, 1, e, share == e, my_row, to_col))
    landings = (across, beside, behind)

    for d, kind, e, sends, to_row, to_col in messages:
        sign = SIGNS[d]
        place = (d * 3 + kind) * half + e - 1

        @pl.when(sends)
        def _():
            def gather(i, carry):
                theirs = to_row + row_count * i
                shift = sign * e if kind == 0 else sign * (e - run)
                other = (theirs + shift + tiles) % tiles
                source = tile_of(d, theirs, other) if kind == 1 else tile_of(d, other, theirs)
                pltpu.make_async_copy(source, fold_out.at[place, i], gather_sem.at[place]).start()
                return carry

            lax.fori_loop(0, slots, gather, 0)

    greet_all(me, peers, device)
    own_list = pltpu.make_async_copy(lists, held.at[me], list_own)
    own_list.start()

    def list_start(hop, carry):
        pltpu.make_async_remote_copy(
            src_ref=lists, dst_ref=held.at[me], send_sem=list_send, recv_sem=list_recv,
            device_id=device((me + hop) % peers), device_id_type=MESH,
        ).start()
        return carry

    lax.fori_loop(1, peers, list_start, 0)

    for d, kind, e, sends, to_row, to_col in messages:
        place = (d * 3 + kind) * half + e - 1

        @pl.when(sends)
        def _():
            wait_bytes(fold_out.at[place], gather_sem.at[place])
            pltpu.make_async_remote_copy(
                src_ref=fold_out.at[place], dst_ref=landings[kind].at[d],
                send_sem=fold_send.at[place], recv_sem=fold_recv.at[d * 3 + kind],
                device_id=(to_row, to_col), device_id_type=MESH,
            ).start()

    for b in range(batches):
        for j in range(run):
            columns = pl.ds(j * TILE, TILE)
            pltpu.make_async_copy(basis.at[b, :, columns], values[b].at[j], basis_sem.at[b]).start()

    for b in range(batches):
        start = begins[b]
        for k in range(run):
            spot = 0
            for j in range(1, run):
                spot = jnp.maximum(spot, jnp.where(tile_list[b, j] == start + k, j, 0))
            order[b, k] = spot

        def table(l, carry):
            for d, sign in enumerate(SIGNS):
                for e in range(width):
                    k = (l - sign * e + run) % run
                    tile_row = (start + k) % row_count
                    tile_col = (tile_row + sign * e + col_count) % col_count
                    last = jnp.maximum(order[b, k], order[b, l])
                    sources[b, d, l * width + e] = tile_row * col_count + tile_col
                    alive[b, d, l * width + e] = jnp.where(last < tile_count[b], 1.0, 0.0)
            return carry

        lax.fori_loop(0, run, table, 0)

    own_list.wait()
    wait_bytes(held.at[pl.ds(0, peers - 1)], list_recv)
    to_scalars = pltpu.make_async_copy(held, starts, list_own)
    to_scalars.start()
    to_scalars.wait()

    def keep(value, d, slot):
        top = jnp.maximum(jnp.max(jnp.abs(value), axis=0, keepdims=True), 1e-30)
        folded[d][slot] = jnp.round(value * (LEVELS / top)).astype(jnp.int32).astype(jnp.int16)
        fold_scales[d][slot] = top * (1.0 / LEVELS)

    def fold(d):
        wait_bytes(near.at[d], near_sem.at[d])

        @pl.when(shares[d] == 0)
        def _():
            def plain(i, carry):
                value = near[d, i].astype(jnp.float32)
                keep(value, d, 2 * i)
                keep(value, d, 2 * i + 1)
                return carry

            lax.fori_loop(0, slots, plain, 0)

        @pl.when(jnp.logical_and(shares[d] >= 1, shares[d] <= half))
        def _():
            for kind in range(3):
                wait_bytes(landings[kind].at[d], fold_recv.at[d * 3 + kind])

            def pair(i, carry):
                keep(near[d, i].astype(jnp.float32) + across[d, i].astype(jnp.float32).T, d, 2 * i)
                keep(beside[d, i].astype(jnp.float32) + behind[d, i].astype(jnp.float32).T, d, 2 * i + 1)
                return carry

            lax.fori_loop(0, slots, pair, 0)

        if col_count > width:

            @pl.when(shares[d] > half)
            def _():
                folded[d][...] = jnp.zeros_like(folded[d])
                fold_scales[d][...] = jnp.zeros_like(fold_scales[d])

    def pack(d):
        sign = SIGNS[d]

        def one(peer, carry):
            for b in range(batches):
                start = starts[peer, 0, b]
                mine = start + (my_row + row_count - start % row_count) % row_count
                slot = jnp.minimum(mine // row_count, slots - 1)
                other = mine + sign * shares[d]
                inside = jnp.logical_and(other >= start, other < start + run)
                index = 2 * slot + jnp.where(inside, 0, 1)
                outbox[d * batches + b][peer] = folded[d][index]
                out_scales[d][peer, b:b + 1, :] = fold_scales[d][index]
            return carry

        lax.fori_loop(0, peers, one, 0)

    def send_scales(d):
        pltpu.make_async_copy(out_scales[d].at[me], land_scales[d].at[me], scale_own.at[d]).start()

        def send(hop, carry):
            to = (me + hop) % peers
            pltpu.make_async_remote_copy(
                src_ref=out_scales[d].at[to], dst_ref=land_scales[d].at[me],
                send_sem=scale_send.at[d], recv_sem=scale_recv.at[d],
                device_id=device(to), device_id_type=MESH,
            ).start()
            return carry

        lax.fori_loop(1, peers, send, 0)

    def send_piece(index):
        pltpu.make_async_copy(outbox[index].at[me], landed[index].at[me], own_sem.at[index]).start()

        def send(hop, carry):
            to = (me + peers // 2 + hop - 1 + hop // (peers // 2 + 1)) % peers
            pltpu.make_async_remote_copy(
                src_ref=outbox[index].at[to], dst_ref=landed[index].at[me],
                send_sem=send_sem.at[index], recv_sem=recv_sem.at[index],
                device_id=device(to), device_id_type=MESH,
            ).start()
            return carry

        lax.fori_loop(1, peers, send, 0)

    def compute(index):
        b, d = pieces[index]
        sign = SIGNS[d]

        for l in range(run):
            for e in range(width):
                peer = sources[b, d, l * width + e]
                scale = land_scales[d][peer, b:b + 1, :] * alive[b, d, l * width + e]
                tile = landed[index][peer].astype(jnp.int32).astype(jnp.float32) * scale
                high = tile.astype(jnp.bfloat16)
                low = (tile - high.astype(jnp.float32)).astype(jnp.bfloat16)
                blocks[l, e * TILE:(e + 1) * TILE, 0:TILE] = high
                blocks[l, e * TILE:(e + 1) * TILE, TILE:2 * TILE] = low

        def some(c, carry):
            begin = pl.multiple_of(c * chunk, chunk)
            rows = pl.ds(begin, chunk)
            parts = [values[b][order[b, k], rows, :] for k in range(run)]
            total = None
            for l in range(run):
                product = jnp.dot(
                    jnp.concatenate([parts[(l - sign * e) % run] for e in range(width)], axis=1),
                    blocks[l], preferred_element_type=jnp.float32,
                )
                term = (product[:, 0:TILE] + product[:, TILE:2 * TILE]) * parts[l].astype(jnp.float32)
                total = term if total is None else total + term
            line = jnp.sum(total.T, axis=0, keepdims=True)
            spot = begin + lax.broadcasted_iota(jnp.int32, (1, chunk), 1)
            line = jnp.where(spot < point_count[b], line, 0.0)
            density[d, b:b + 1, rows] = line
            x = offsets[0, b:b + 1, rows]
            y = offsets[1, b:b + 1, rows]
            z = offsets[2, b:b + 1, rows]
            w = weights[b:b + 1, rows]
            r2 = x * x + y * y + z * z
            weighted = [
                w, w * x, w * y, w * z, w * (x * y), w * (y * z),
                w * (3.0 * z * z - r2), w * (x * z), w * (x * x - y * y),
            ]
            terms = [line * item for item in weighted]
            terms += [jnp.zeros((1, chunk), jnp.float32)] * (SLOT - len(terms))
            stacked = jnp.concatenate(terms, axis=0)
            base = (me * batches + b) * stride
            atom = (atoms[b:b + 1, rows] - base + ATOMS) % ATOMS
            for j in range(SPREAD):
                chosen = jnp.where(atom == j, stacked, 0.0)
                partial = None
                for q in range(chunk // TILE):
                    part = chosen[:, q * TILE:(q + 1) * TILE]
                    partial = part if partial is None else partial + part
                at_rows = pl.ds(j * SLOT, SLOT)
                sums[index, at_rows, :] = sums[index, at_rows, :] + partial
            return carry

        lax.fori_loop(0, points // chunk, some, 0)

    sums[...] = jnp.zeros_like(sums)
    for d in range(2):
        fold(d)
        pack(d)
        send_scales(d)
        for b in range(batches):
            send_piece(d * batches + b)

    for b in range(batches):
        wait_bytes(values[b], basis_sem.at[b])
    for index, (b, d) in enumerate(pieces):
        if b == 0:
            pltpu.make_async_copy(out_scales[d].at[me], land_scales[d].at[me], scale_own.at[d]).wait()
            wait_bytes(land_scales[d].at[pl.ds(0, peers - 1)], scale_recv.at[d])
        pltpu.make_async_copy(outbox[index].at[me], landed[index].at[me], own_sem.at[index]).wait()
        wait_bytes(landed[index].at[pl.ds(0, peers - 1)], recv_sem.at[index])
        compute(index)

    for index in range(len(pieces)):
        stage[index:index + 1, :] = jnp.sum(sums[index].T, axis=0, keepdims=True)
    for index in range(len(pieces)):
        wait_bytes(landed[index].at[pl.ds(0, peers - 1)], send_sem.at[index])
    for d in range(2):
        wait_bytes(land_scales[d].at[pl.ds(0, peers - 1)], scale_send.at[d])
    wait_bytes(held.at[pl.ds(0, peers - 1)], list_send)

    def last_start(hop, carry):
        pltpu.make_async_remote_copy(
            src_ref=stage, dst_ref=gathered.at[me], send_sem=last_send, recv_sem=last_recv,
            device_id=device((me + hop) % peers), device_id_type=MESH,
        ).start()
        return carry

    lax.fori_loop(1, peers, last_start, 0)
    last = pltpu.make_async_copy(stage, gathered.at[me], last_own)
    last.start()
    for d, kind, e, sends, to_row, to_col in messages:
        place = (d * 3 + kind) * half + e - 1

        @pl.when(sends)
        def _():
            wait_bytes(near.at[d], fold_send.at[place])

    last.wait()
    wait_bytes(gathered.at[pl.ds(0, peers - 1)], last_recv)
    every[...] = gathered[...]
    wait_bytes(gathered.at[pl.ds(0, peers - 1)], last_send)


def density_of(
    tile_list, tile_count, point_count, first, second, basis, offsets, weights, atoms,
    row_count, col_count,
):
    batches, points, span = basis.shape
    run = span // TILE
    half = run // 2
    peers = row_count * col_count
    slots = first.shape[0] // TILE
    pieces = 2 * batches
    whole = pl.BlockSpec(memory_space=pltpu.VMEM)
    scalar = pl.BlockSpec(memory_space=pltpu.SMEM)
    anywhere = pl.BlockSpec(memory_space=pl.ANY)
    copies = pltpu.SemaphoreType.DMA
    return pl.pallas_call(
        functools.partial(main_kernel, run, row_count, col_count),
        out_shape=[
            jax.ShapeDtypeStruct((2, batches, points), jnp.float32),
            jax.ShapeDtypeStruct((peers, pieces, SPREAD * SLOT), jnp.float32),
        ],
        in_specs=[scalar] * 3 + [anywhere] * 3 + [whole] * 3,
        out_specs=[whole, whole],
        scratch_shapes=[pltpu.VMEM((run, points, TILE), basis.dtype)] * batches
        + [pltpu.VMEM((peers, TILE, TILE), jnp.int16)] * (2 * pieces)
        + [pltpu.VMEM((2 * slots, TILE, TILE), jnp.int16)] * 2
        + [pltpu.VMEM((2 * slots, 1, TILE), jnp.float32)] * 2
        + [pltpu.VMEM((peers, batches, TILE), jnp.float32)] * 4
        + [
            pltpu.SMEM((batches, 2, run * (half + 1)), jnp.int32),
            pltpu.SMEM((batches, 2, run * (half + 1)), jnp.float32),
            pltpu.SMEM((batches, run), jnp.int32),
            pltpu.VMEM((1, TILE), jnp.int32),
            pltpu.VMEM((6 * half, slots, TILE, TILE), first.dtype),
            copies((6 * half,)),
        ]
        + [pltpu.VMEM((2, slots, TILE, TILE), first.dtype)] * 4
        + [
            pltpu.VMEM((peers, 1, TILE), jnp.int32),
            pltpu.SMEM((peers, 1, TILE), jnp.int32),
            pltpu.VMEM((run, (half + 1) * TILE, 2 * TILE), jnp.bfloat16),
            pltpu.VMEM((pieces, SPREAD * SLOT, TILE), jnp.float32),
            pltpu.VMEM((pieces, SPREAD * SLOT), jnp.float32),
            pltpu.VMEM((peers, pieces, SPREAD * SLOT), jnp.float32),
            copies((2,)), copies((6,)), copies((6 * half,)), copies, copies, copies,
            copies((batches,)), copies((pieces,)), copies((pieces,)), copies((pieces,)),
            copies((2,)), copies((2,)), copies((2,)), copies, copies, copies,
        ],
        compiler_params=pltpu.CompilerParams(
            collective_id=0, has_side_effects=True, vmem_limit_bytes=62 * 1024 * 1024
        ),
        name="density",
    )(tile_list, tile_count, point_count, first, second, basis, offsets, weights, atoms)


def local(
    density_first, density_second, basis, tile_list, tile_count, point_count, offsets, weights,
    atom_of_point,
):
    row_count = lax.axis_size("row")
    col_count = lax.axis_size("col")
    peers = row_count * col_count
    batches = tile_list.shape[0]
    density, every = density_of(
        tile_list, tile_count, point_count, density_first, density_second, basis, offsets,
        weights, atom_of_point, row_count, col_count,
    )
    stride = ATOMS // (peers * batches)
    every = every.reshape(peers, 2, batches, SPREAD, SLOT)[..., :TERMS]
    every = every.transpose(1, 4, 0, 2, 3).reshape(2 * TERMS, peers * batches, SPREAD)
    blocks = -(-SPREAD // stride)
    every = jnp.pad(every, ((0, 0), (0, 0), (0, blocks * stride - SPREAD)))
    total = None
    for q in range(blocks):
        part = every[:, :, q * stride:(q + 1) * stride].reshape(2 * TERMS, ATOMS)
        part = jnp.roll(part, q * stride, axis=1)
        total = part if total is None else total + part
    return density, total.reshape(2, TERMS, ATOMS)


def solution(mesh):
    placed = (
        P("row", "col"),
        P("row", "col"),
        P(("row", "col"), None, None),
        P(("row", "col"), None),
        P(("row", "col")),
        P(("row", "col")),
        P(None, ("row", "col"), None),
        P(("row", "col"), None),
        P(("row", "col"), None),
    )
    return jax.shard_map(
        local,
        mesh=mesh,
        in_specs=placed,
        out_specs=(P(None, ("row", "col"), None), P()),
        check_vma=False,
    )
```

```python
import functools

import jax
import jax.numpy as jnp
from jax import lax
from jax.experimental import pallas as pl
from jax.experimental.pallas import tpu as pltpu
from jax.sharding import PartitionSpec as P

TILE = 128
ATOMS = 1024
SPREAD = 8
TERMS = 9
SLOT = 16
SIGNS = (1, -1)
LEVELS = 32767.0
MESH = pl.DeviceIdType.MESH


def greet_all(me, peers, device):
    barrier = pltpu.get_barrier_semaphore()

    def greet(hop, carry):
        pl.semaphore_signal(
            barrier, inc=1, device_id=device((me + hop) % peers), device_id_type=MESH
        )
        return carry

    lax.fori_loop(1, peers, greet, 0)
    pl.semaphore_wait(barrier, peers - 1)


def main_kernel(
    run, row_count, col_count, tile_list, tile_count, point_count, first, second, basis,
    offsets, weights, atoms, density, every, *scratch,
):
    batches, points = weights.shape
    pieces = [(b, d) for d in range(2) for b in range(batches)]
    values, scratch = scratch[:batches], scratch[batches:]
    outbox, scratch = scratch[:len(pieces)], scratch[len(pieces):]
    landed, scratch = scratch[:len(pieces)], scratch[len(pieces):]
    folded, fold_scales, out_scales, land_scales, scratch = (
        scratch[0:2], scratch[2:4], scratch[4:6], scratch[6:8], scratch[8:]
    )
    (
        sources, alive, order, lists, fold_out, gather_sem,
        near, across, beside, behind, held, starts, blocks, sums, stage, gathered,
        near_sem, fold_recv, fold_send, list_send, list_recv, list_own, basis_sem,
        send_sem, recv_sem, own_sem, scale_send, scale_recv, scale_own,
        last_send, last_recv, last_own,
    ) = scratch
    half = run // 2
    width = half + 1
    peers = row_count * col_count
    my_row = lax.axis_index("row")
    my_col = lax.axis_index("col")
    me = my_row * col_count + my_col
    matrices = (first, second)
    slots = near.shape[1]
    tiles = slots * row_count
    chunk = min(512, points)
    stride = ATOMS // (peers * batches)
    shares = [(sign * (my_col - my_row) + row_count * col_count) % col_count for sign in SIGNS]

    def device(index):
        return (index // col_count, index % col_count)

    def wait_bytes(ref, sem):
        pltpu.make_async_copy(ref, ref, sem).wait()

    def tile_of(d, tile_row, tile_col):
        rows = pl.ds(pl.multiple_of((tile_row // row_count) * TILE, TILE), TILE)
        cols = pl.ds(pl.multiple_of((tile_col // col_count) * TILE, TILE), TILE)
        return matrices[d].at[rows, cols]

    for d, sign in enumerate(SIGNS):

        def take(i, carry):
            mine = my_row + row_count * i
            other = (mine + sign * shares[d] + tiles) % tiles
            pltpu.make_async_copy(tile_of(d, mine, other), near.at[d, i], near_sem.at[d]).start()
            return carry

        lax.fori_loop(0, slots, take, 0)

    lane = lax.broadcasted_iota(jnp.int32, lists.shape, 1)
    firsts = jnp.zeros(lists.shape, jnp.int32)
    begins = []
    for b in range(batches):
        begins.append(functools.reduce(jnp.minimum, [tile_list[b, j] for j in range(run)]))
        firsts = jnp.where(lane == b, begins[b], firsts)
    lists[...] = firsts

    messages = []
    for d, sign in enumerate(SIGNS):
        for e in range(1, half + 1):
            for kind, shift in ((0, sign * e), (2, sign * (e - run))):
                to_row = (my_row - shift + 2 * row_count) % row_count
                to_col = (to_row + sign * e + col_count) % col_count
                messages.append((d, kind, e, to_row % col_count == my_col, to_row, to_col))
        for e in range(1, half + 1):
            to_col = (my_col + sign * run + 2 * run * col_count) % col_count
            share = (sign * (to_col - my_row) + row_count * col_count) % col_count
            messages.append((d, 1, e, share == e, my_row, to_col))
    landings = (across, beside, behind)

    for d, kind, e, sends, to_row, to_col in messages:
        sign = SIGNS[d]
        place = (d * 3 + kind) * half + e - 1

        @pl.when(sends)
        def _():
            def gather(i, carry):
                theirs = to_row + row_count * i
                shift = sign * e if kind == 0 else sign * (e - run)
                other = (theirs + shift + tiles) % tiles
                source = tile_of(d, theirs, other) if kind == 1 else tile_of(d, other, theirs)
                pltpu.make_async_copy(source, fold_out.at[place, i], gather_sem.at[place]).start()
                return carry

            lax.fori_loop(0, slots, gather, 0)

    greet_all(me, peers, device)
    own_list = pltpu.make_async_copy(lists, held.at[me], list_own)
    own_list.start()

    def list_start(hop, carry):
        pltpu.make_async_remote_copy(
            src_ref=lists, dst_ref=held.at[me], send_sem=list_send, recv_sem=list_recv,
            device_id=device((me + hop) % peers), device_id_type=MESH,
        ).start()
        return carry

    lax.fori_loop(1, peers, list_start, 0)

    for d, kind, e, sends, to_row, to_col in messages:
        place = (d * 3 + kind) * half + e - 1

        @pl.when(sends)
        def _():
            wait_bytes(fold_out.at[place], gather_sem.at[place])
            pltpu.make_async_remote_copy(
                src_ref=fold_out.at[place], dst_ref=landings[kind].at[d],
                send_sem=fold_send.at[place], recv_sem=fold_recv.at[d * 3 + kind],
                device_id=(to_row, to_col), device_id_type=MESH,
            ).start()

    for b in range(batches):
        for j in range(run):
            columns = pl.ds(j * TILE, TILE)
            pltpu.make_async_copy(basis.at[b, :, columns], values[b].at[j], basis_sem.at[b]).start()

    for b in range(batches):
        start = begins[b]
        for k in range(run):
            spot = 0
            for j in range(1, run):
                spot = jnp.maximum(spot, jnp.where(tile_list[b, j] == start + k, j, 0))
            order[b, k] = spot

        def table(l, carry):
            for d, sign in enumerate(SIGNS):
                for e in range(width):
                    k = (l - sign * e + run) % run
                    tile_row = (start + k) % row_count
                    tile_col = (tile_row + sign * e + col_count) % col_count
                    last = jnp.maximum(order[b, k], order[b, l])
                    sources[b, d, l * width + e] = tile_row * col_count + tile_col
                    alive[b, d, l * width + e] = jnp.where(last < tile_count[b], 1.0, 0.0)
            return carry

        lax.fori_loop(0, run, table, 0)

    own_list.wait()
    wait_bytes(held.at[pl.ds(0, peers - 1)], list_recv)
    to_scalars = pltpu.make_async_copy(held, starts, list_own)
    to_scalars.start()
    to_scalars.wait()

    def keep(value, d, slot):
        top = jnp.maximum(jnp.max(jnp.abs(value), axis=0, keepdims=True), 1e-30)
        folded[d][slot] = jnp.round(value * (LEVELS / top)).astype(jnp.int32).astype(jnp.int16)
        fold_scales[d][slot] = top * (1.0 / LEVELS)

    def fold(d):
        wait_bytes(near.at[d], near_sem.at[d])

        @pl.when(shares[d] == 0)
        def _():
            def plain(i, carry):
                value = near[d, i].astype(jnp.float32)
                keep(value, d, 2 * i)
                keep(value, d, 2 * i + 1)
                return carry

            lax.fori_loop(0, slots, plain, 0)

        @pl.when(jnp.logical_and(shares[d] >= 1, shares[d] <= half))
        def _():
            for kind in range(3):
                wait_bytes(landings[kind].at[d], fold_recv.at[d * 3 + kind])

            def pair(i, carry):
                keep(near[d, i].astype(jnp.float32) + across[d, i].astype(jnp.float32).T, d, 2 * i)
                keep(beside[d, i].astype(jnp.float32) + behind[d, i].astype(jnp.float32).T, d, 2 * i + 1)
                return carry

            lax.fori_loop(0, slots, pair, 0)

        if col_count > width:

            @pl.when(shares[d] > half)
            def _():
                folded[d][...] = jnp.zeros_like(folded[d])
                fold_scales[d][...] = jnp.zeros_like(fold_scales[d])

    def pack(d):
        sign = SIGNS[d]

        def one(peer, carry):
            for b in range(batches):
                start = starts[peer, 0, b]
                mine = start + (my_row + row_count - start % row_count) % row_count
                slot = jnp.minimum(mine // row_count, slots - 1)
                other = mine + sign * shares[d]
                inside = jnp.logical_and(other >= start, other < start + run)
                index = 2 * slot + jnp.where(inside, 0, 1)
                outbox[d * batches + b][peer] = folded[d][index]
                out_scales[d][peer, b:b + 1, :] = fold_scales[d][index]
            return carry

        lax.fori_loop(0, peers, one, 0)

    def send_scales(d):
        pltpu.make_async_copy(out_scales[d].at[me], land_scales[d].at[me], scale_own.at[d]).start()

        def send(hop, carry):
            to = (me + hop) % peers
            pltpu.make_async_remote_copy(
                src_ref=out_scales[d].at[to], dst_ref=land_scales[d].at[me],
                send_sem=scale_send.at[d], recv_sem=scale_recv.at[d],
                device_id=device(to), device_id_type=MESH,
            ).start()
            return carry

        lax.fori_loop(1, peers, send, 0)

    def send_piece(index):
        pltpu.make_async_copy(outbox[index].at[me], landed[index].at[me], own_sem.at[index]).start()

        def send(hop, carry):
            near_by = hop // (peers // 2 + 1)
            place = (me + hop - 1 + near_by) % (peers // 2)
            to = (((me // (peers // 2)) + 1 + near_by) % 2) * (peers // 2) + place
            pltpu.make_async_remote_copy(
                src_ref=outbox[index].at[to], dst_ref=landed[index].at[me],
                send_sem=send_sem.at[index], recv_sem=recv_sem.at[index],
                device_id=device(to), device_id_type=MESH,
            ).start()
            return carry

        lax.fori_loop(1, peers, send, 0)

    def compute(index):
        b, d = pieces[index]
        sign = SIGNS[d]

        for l in range(run):
            for e in range(width):
                peer = sources[b, d, l * width + e]
                scale = land_scales[d][peer, b:b + 1, :] * alive[b, d, l * width + e]
                tile = landed[index][peer].astype(jnp.int32).astype(jnp.float32) * scale
                high = tile.astype(jnp.bfloat16)
                low = (tile - high.astype(jnp.float32)).astype(jnp.bfloat16)
                blocks[l, e * TILE:(e + 1) * TILE, 0:TILE] = high
                blocks[l, e * TILE:(e + 1) * TILE, TILE:2 * TILE] = low

        def some(c, carry):
            begin = pl.multiple_of(c * chunk, chunk)
            rows = pl.ds(begin, chunk)
            parts = [values[b][order[b, k], rows, :] for k in range(run)]
            total = None
            for l in range(run):
                product = jnp.dot(
                    jnp.concatenate([parts[(l - sign * e) % run] for e in range(width)], axis=1),
                    blocks[l], preferred_element_type=jnp.float32,
                )
                term = (product[:, 0:TILE] + product[:, TILE:2 * TILE]) * parts[l].astype(jnp.float32)
                total = term if total is None else total + term
            line = jnp.sum(total.T, axis=0, keepdims=True)
            spot = begin + lax.broadcasted_iota(jnp.int32, (1, chunk), 1)
            line = jnp.where(spot < point_count[b], line, 0.0)
            density[d, b:b + 1, rows] = line
            x = offsets[0, b:b + 1, rows]
            y = offsets[1, b:b + 1, rows]
            z = offsets[2, b:b + 1, rows]
            w = weights[b:b + 1, rows]
            r2 = x * x + y * y + z * z
            weighted = [
                w, w * x, w * y, w * z, w * (x * y), w * (y * z),
                w * (3.0 * z * z - r2), w * (x * z), w * (x * x - y * y),
            ]
            terms = [line * item for item in weighted]
            terms += [jnp.zeros((1, chunk), jnp.float32)] * (SLOT - len(terms))
            stacked = jnp.concatenate(terms, axis=0)
            base = (me * batches + b) * stride
            atom = (atoms[b:b + 1, rows] - base + ATOMS) % ATOMS
            for j in range(SPREAD):
                chosen = jnp.where(atom == j, stacked, 0.0)
                partial = None
                for q in range(chunk // TILE):
                    part = chosen[:, q * TILE:(q + 1) * TILE]
                    partial = part if partial is None else partial + part
                at_rows = pl.ds(j * SLOT, SLOT)
                sums[index, at_rows, :] = sums[index, at_rows, :] + partial
            return carry

        lax.fori_loop(0, points // chunk, some, 0)

    sums[...] = jnp.zeros_like(sums)
    for d in range(2):
        fold(d)
        pack(d)
        send_scales(d)
        for b in range(batches):
            send_piece(d * batches + b)

    for b in range(batches):
        wait_bytes(values[b], basis_sem.at[b])
    for index, (b, d) in enumerate(pieces):
        if b == 0:
            pltpu.make_async_copy(out_scales[d].at[me], land_scales[d].at[me], scale_own.at[d]).wait()
            wait_bytes(land_scales[d].at[pl.ds(0, peers - 1)], scale_recv.at[d])
        pltpu.make_async_copy(outbox[index].at[me], landed[index].at[me], own_sem.at[index]).wait()
        wait_bytes(landed[index].at[pl.ds(0, peers - 1)], recv_sem.at[index])
        compute(index)

    for index in range(len(pieces)):
        stage[index:index + 1, :] = jnp.sum(sums[index].T, axis=0, keepdims=True)
    for index in range(len(pieces)):
        wait_bytes(landed[index].at[pl.ds(0, peers - 1)], send_sem.at[index])
    for d in range(2):
        wait_bytes(land_scales[d].at[pl.ds(0, peers - 1)], scale_send.at[d])
    wait_bytes(held.at[pl.ds(0, peers - 1)], list_send)

    def last_start(hop, carry):
        pltpu.make_async_remote_copy(
            src_ref=stage, dst_ref=gathered.at[me], send_sem=last_send, recv_sem=last_recv,
            device_id=device((me + hop) % peers), device_id_type=MESH,
        ).start()
        return carry

    lax.fori_loop(1, peers, last_start, 0)
    last = pltpu.make_async_copy(stage, gathered.at[me], last_own)
    last.start()
    for d, kind, e, sends, to_row, to_col in messages:
        place = (d * 3 + kind) * half + e - 1

        @pl.when(sends)
        def _():
            wait_bytes(near.at[d], fold_send.at[place])

    last.wait()
    wait_bytes(gathered.at[pl.ds(0, peers - 1)], last_recv)
    every[...] = gathered[...]
    wait_bytes(gathered.at[pl.ds(0, peers - 1)], last_send)


def density_of(
    tile_list, tile_count, point_count, first, second, basis, offsets, weights, atoms,
    row_count, col_count,
):
    batches, points, span = basis.shape
    run = span // TILE
    half = run // 2
    peers = row_count * col_count
    slots = first.shape[0] // TILE
    pieces = 2 * batches
    whole = pl.BlockSpec(memory_space=pltpu.VMEM)
    scalar = pl.BlockSpec(memory_space=pltpu.SMEM)
    anywhere = pl.BlockSpec(memory_space=pl.ANY)
    copies = pltpu.SemaphoreType.DMA
    return pl.pallas_call(
        functools.partial(main_kernel, run, row_count, col_count),
        out_shape=[
            jax.ShapeDtypeStruct((2, batches, points), jnp.float32),
            jax.ShapeDtypeStruct((peers, pieces, SPREAD * SLOT), jnp.float32),
        ],
        in_specs=[scalar] * 3 + [anywhere] * 3 + [whole] * 3,
        out_specs=[whole, whole],
        scratch_shapes=[pltpu.VMEM((run, points, TILE), basis.dtype)] * batches
        + [pltpu.VMEM((peers, TILE, TILE), jnp.int16)] * (2 * pieces)
        + [pltpu.VMEM((2 * slots, TILE, TILE), jnp.int16)] * 2
        + [pltpu.VMEM((2 * slots, 1, TILE), jnp.float32)] * 2
        + [pltpu.VMEM((peers, batches, TILE), jnp.float32)] * 4
        + [
            pltpu.SMEM((batches, 2, run * (half + 1)), jnp.int32),
            pltpu.SMEM((batches, 2, run * (half + 1)), jnp.float32),
            pltpu.SMEM((batches, run), jnp.int32),
            pltpu.VMEM((1, TILE), jnp.int32),
            pltpu.VMEM((6 * half, slots, TILE, TILE), first.dtype),
            copies((6 * half,)),
        ]
        + [pltpu.VMEM((2, slots, TILE, TILE), first.dtype)] * 4
        + [
            pltpu.VMEM((peers, 1, TILE), jnp.int32),
            pltpu.SMEM((peers, 1, TILE), jnp.int32),
            pltpu.VMEM((run, (half + 1) * TILE, 2 * TILE), jnp.bfloat16),
            pltpu.VMEM((pieces, SPREAD * SLOT, TILE), jnp.float32),
            pltpu.VMEM((pieces, SPREAD * SLOT), jnp.float32),
            pltpu.VMEM((peers, pieces, SPREAD * SLOT), jnp.float32),
            copies((2,)), copies((6,)), copies((6 * half,)), copies, copies, copies,
            copies((batches,)), copies((pieces,)), copies((pieces,)), copies((pieces,)),
            copies((2,)), copies((2,)), copies((2,)), copies, copies, copies,
        ],
        compiler_params=pltpu.CompilerParams(
            collective_id=0, has_side_effects=True, vmem_limit_bytes=62 * 1024 * 1024
        ),
        name="density",
    )(tile_list, tile_count, point_count, first, second, basis, offsets, weights, atoms)


def local(
    density_first, density_second, basis, tile_list, tile_count, point_count, offsets, weights,
    atom_of_point,
):
    row_count = lax.axis_size("row")
    col_count = lax.axis_size("col")
    peers = row_count * col_count
    batches = tile_list.shape[0]
    density, every = density_of(
        tile_list, tile_count, point_count, density_first, density_second, basis, offsets,
        weights, atom_of_point, row_count, col_count,
    )
    stride = ATOMS // (peers * batches)
    every = every.reshape(peers, 2, batches, SPREAD, SLOT)[..., :TERMS]
    every = every.transpose(1, 4, 0, 2, 3).reshape(2 * TERMS, peers * batches, SPREAD)
    blocks = -(-SPREAD // stride)
    every = jnp.pad(every, ((0, 0), (0, 0), (0, blocks * stride - SPREAD)))
    total = None
    for q in range(blocks):
        part = every[:, :, q * stride:(q + 1) * stride].reshape(2 * TERMS, ATOMS)
        part = jnp.roll(part, q * stride, axis=1)
        total = part if total is None else total + part
    return density, total.reshape(2, TERMS, ATOMS)


def solution(mesh):
    placed = (
        P("row", "col"),
        P("row", "col"),
        P(("row", "col"), None, None),
        P(("row", "col"), None),
        P(("row", "col")),
        P(("row", "col")),
        P(None, ("row", "col"), None),
        P(("row", "col"), None),
        P(("row", "col"), None),
    )
    return jax.shard_map(
        local,
        mesh=mesh,
        in_specs=placed,
        out_specs=(P(None, ("row", "col"), None), P()),
        check_vma=False,
    )
```
